128 devices in a mesh: batch: 1, tree: 128 (over z, y, x, core).
Axes of the slice: x: 4, y: 4, z: 4, core: 2. Of those that a mesh axis runs over, the one named last changes fastest.
Arguments:
- x_vecs: float32 [262144, 512], P(('batch', 'tree'))
- d_near: bfloat16 [1024, 256, 256], P('tree')
- u_leaf: bfloat16 [1024, 256, 64], P('tree')
- v_leaf: bfloat16 [1024, 256, 64], P('tree')
- w_h0: bfloat16 [1024, 64, 128], P('tree')
- r_h0: bfloat16 [1024, 64, 128], P('tree')
- b_h0: bfloat16 [1024, 64, 64], P('tree')
- w_h1: bfloat16 [512, 128, 128], P('tree')
- r_h1: bfloat16 [512, 128, 128], P('tree')
- b_h1: bfloat16 [512, 128, 128], P('tree')
- w_h2: bfloat16 [256, 128, 256], P('tree')
- r_h2: bfloat16 [256, 128, 256], P('tree')
- b_h2: bfloat16 [256, 128, 128], P('tree')
- w_upper: bfloat16 [128, 256, 256], P('tree')
- r_upper: bfloat16 [128, 256, 256], P('tree')
- b_upper: bfloat16 [128, 256, 256], P('tree')
- w_top: bfloat16 [124, 256, 256], replicated
- r_top: bfloat16 [124, 256, 256], replicated
- b_top: bfloat16 [126, 256, 256], replicated
Outputs:
- output: float32 [262144, 512], P(('batch', 'tree'))
All inputs are finite; a program needn't handle non-finite values.
Results may differ from the reference program's by a relative error of at most 0.0158533.
Values are sent between devices in bfloat16 or wider.
A program may use at most 1 GiB of HBM per device.

```python
import math
import jax
import jax.numpy as jnp
from jax import lax

LEAF_SIZE = 256
LEAF_RANK = 64
NUM_RHS = 512
LEAVES_DEV = 8
TREE_DEVS = 128

LEAF_COUNT = TREE_DEVS * LEAVES_DEV
ROW_COUNT = LEAF_COUNT * LEAF_SIZE
UPPER_DEV = LEAVES_DEV // 4 - 1
TOP_DEPTH = int(math.log2(TREE_DEVS) + 0.5)
UPPER_DEPTH = int(math.log2(UPPER_DEV + 1) + 0.5)


def draw_normal(key, shape, scale):
    return (jax.random.normal(key, shape, jnp.float32) * scale).astype(jnp.bfloat16)


def setup_inputs(seed: int = 0, part: int = 0) -> dict:
    keys = jax.random.split(jax.random.key(seed), 18)
    x_key = jax.random.fold_in(jax.random.key(seed + 1), part)
    rank_one = LEAF_RANK
    rank_two = 2 * LEAF_RANK
    rank_four = 4 * LEAF_RANK
    upper_rows = TREE_DEVS * UPPER_DEV
    return {
        'x_vecs': jax.random.normal(x_key, (ROW_COUNT, NUM_RHS), jnp.float32),
        'd_near': draw_normal(keys[0], (LEAF_COUNT, LEAF_SIZE, LEAF_SIZE), LEAF_SIZE ** -0.5),
        'u_leaf': draw_normal(keys[1], (LEAF_COUNT, LEAF_SIZE, rank_one), rank_one ** -0.5),
        'v_leaf': draw_normal(keys[2], (LEAF_COUNT, LEAF_SIZE, rank_one), LEAF_SIZE ** -0.5),
        'w_h0': draw_normal(keys[3], (LEAF_COUNT, rank_one, rank_two), (2 * rank_one) ** -0.5),
        'r_h0': draw_normal(keys[4], (LEAF_COUNT, rank_one, rank_two), rank_two ** -0.5),
        'b_h0': draw_normal(keys[5], (LEAF_COUNT, rank_one, rank_one), rank_one ** -0.5),
        'w_h1': draw_normal(keys[6], (LEAF_COUNT // 2, rank_two, rank_two), (2 * rank_two) ** -0.5),
        'r_h1': draw_normal(keys[7], (LEAF_COUNT // 2, rank_two, rank_two), rank_two ** -0.5),
        'b_h1': draw_normal(keys[8], (LEAF_COUNT // 2, rank_two, rank_two), rank_two ** -0.5),
        'w_h2': draw_normal(keys[9], (LEAF_COUNT // 4, rank_two, rank_four), (2 * rank_two) ** -0.5),
        'r_h2': draw_normal(keys[10], (LEAF_COUNT // 4, rank_two, rank_four), rank_four ** -0.5),
        'b_h2': draw_normal(keys[11], (LEAF_COUNT // 4, rank_two, rank_two), rank_two ** -0.5),
        'w_upper': draw_normal(keys[12], (upper_rows, rank_four, rank_four), (2 * rank_four) ** -0.5),
        'r_upper': draw_normal(keys[13], (upper_rows, rank_four, rank_four), rank_four ** -0.5),
        'b_upper': draw_normal(keys[14], (upper_rows, rank_four, rank_four), rank_four ** -0.5),
        'w_top': draw_normal(keys[15], (TREE_DEVS - 4, rank_four, rank_four), (2 * rank_four) ** -0.5),
        'r_top': draw_normal(keys[16], (TREE_DEVS - 4, rank_four, rank_four), rank_four ** -0.5),
        'b_top': draw_normal(keys[17], (TREE_DEVS - 2, rank_four, rank_four), rank_four ** -0.5),
    }


def merge_up(w_child, x_child):
    prod = jnp.einsum('nkq,nkc->nqc', w_child.astype(jnp.float32), x_child.astype(jnp.float32))
    pairs = prod.reshape(prod.shape[0] // 2, 2, prod.shape[1], prod.shape[2])
    return (pairs[:, 0] + pairs[:, 1]).astype(jnp.bfloat16)


def couple(b_node, x_level):
    pairs = x_level.reshape(x_level.shape[0] // 2, 2, x_level.shape[1], x_level.shape[2])
    swapped = jnp.flip(pairs, axis=1).reshape(x_level.shape)
    return jnp.einsum('nkj,njc->nkc', b_node.astype(jnp.float32), swapped.astype(jnp.float32))


def push_down(r_child, y_parent, coupled):
    r_pairs = r_child.reshape(r_child.shape[0] // 2, 2, r_child.shape[1], r_child.shape[2])
    prod = jnp.einsum('nekq,nqc->nekc', r_pairs.astype(jnp.float32), y_parent.astype(jnp.float32))
    return (coupled + prod.reshape(coupled.shape)).astype(jnp.bfloat16)


def upper_levels(packed):
    grouped = packed.reshape(TREE_DEVS, UPPER_DEV, packed.shape[1], packed.shape[2])
    return [grouped[:, 2 ** step - 1:2 ** (step + 1) - 1].reshape(TREE_DEVS * 2 ** step, packed.shape[1], packed.shape[2]) for step in range(UPPER_DEPTH)]


def top_levels(packed, first):
    return [packed[2 ** level - 2 ** first:2 ** (level + 1) - 2 ** first] for level in range(first, TOP_DEPTH)]


def reference(x_vecs, d_near, u_leaf, v_leaf, w_h0, r_h0, b_h0, w_h1, r_h1, b_h1, w_h2, r_h2, b_h2, w_upper, r_upper, b_upper, w_top, r_top, b_top):
    x_dev = x_vecs.astype(jnp.bfloat16).reshape(TREE_DEVS, LEAVES_DEV, LEAF_SIZE, NUM_RHS)

    def leaf_up(block):
        v_block, x_block = block
        prod = jnp.einsum('lmk,lmc->lkc', v_block.astype(jnp.float32), x_block.astype(jnp.float32))
        return prod.astype(jnp.bfloat16)

    x_skel = lax.map(leaf_up, (v_leaf.reshape(TREE_DEVS, LEAVES_DEV, LEAF_SIZE, LEAF_RANK), x_dev))
    skel_up = [x_skel.reshape(LEAF_COUNT, LEAF_RANK, NUM_RHS)]
    w_levels = [w_h0, w_h1, w_h2] + list(reversed(upper_levels(w_upper))) + list(reversed(top_levels(w_top, 2)))
    r_levels = [r_h0, r_h1, r_h2] + list(reversed(upper_levels(r_upper))) + list(reversed(top_levels(r_top, 2)))
    b_levels = [b_h0, b_h1, b_h2] + list(reversed(upper_levels(b_upper))) + list(reversed(top_levels(b_top, 1)))
    for w_child in w_levels:
        skel_up.append(merge_up(w_child, skel_up[-1]))
    coupled = [couple(b_node, x_level) for b_node, x_level in zip(b_levels, skel_up)]
    y_skel = coupled[-1].astype(jnp.bfloat16)
    for level in range(len(r_levels) - 1, -1, -1):
        y_skel = push_down(r_levels[level], y_skel, coupled[level])

    def leaf_down(block):
        d_block, u_block, x_block, y_block = block
        near = jnp.einsum('lmj,ljc->lmc', d_block.astype(jnp.float32), x_block.astype(jnp.float32))
        far = jnp.einsum('lmk,lkc->lmc', u_block.astype(jnp.float32), y_block.astype(jnp.float32))
        return near + far

    y_out = lax.map(leaf_down, (d_near.reshape(TREE_DEVS, LEAVES_DEV, LEAF_SIZE, LEAF_SIZE), u_leaf.reshape(TREE_DEVS, LEAVES_DEV, LEAF_SIZE, LEAF_RANK), x_dev, y_skel.reshape(TREE_DEVS, LEAVES_DEV, LEAF_RANK, NUM_RHS)))
    return y_out.reshape(ROW_COUNT, NUM_RHS)
```

```python
import jax
import jax.numpy as jnp
from jax import lax
from jax.experimental import pallas as pl
from jax.experimental.pallas import tpu as pltpu
from jax.sharding import PartitionSpec as P

F32 = jnp.float32
BF16 = jnp.bfloat16
MESH = pl.DeviceIdType.MESH
COLS = 64


def nn(a, b):
    return lax.dot_general(a, b, (((1,), (0,)), ((), ())), preferred_element_type=F32)


def nt(a, b):
    return lax.dot_general(a, b, (((1,), (1,)), ((), ())), preferred_element_type=F32)


def tn(a, b):
    return lax.dot_general(a, b, (((0,), (0,)), ((), ())), preferred_element_type=F32)


def kernel(x, d, u, v, w0, r0, b0, w1, r1, b1, w2, r2, b2, wu, ru, bu, wt, rt, bt, out,
           xf, xb, dv, uv, vv, w0v, r0v, b0v, w1v, r1v, b1v, w2v, r2v, b2v, wuv, ruv, buv,
           wt6, wt5, wt4, wt3, wt2, rt6, rt5, rt4, rt3, rt2, bt6, bt5, bt4, bt3, bt2, bt1,
           xh0, xh1, xh2, x7, x7s, part, partr, x6h, buf6, x5, x4s, buf4, x3, x2s, buf2, x1,
           g0, g1, g2, g7, g6t, g5t, y6h, yfull, yh0,
           xsem, lsem, wsem, s0, q0, s6, q6, s4, q4, s2, q2, sy, qy, sc, qc):
    me = lax.axis_index('tree')
    core = me % 2
    px = (me // 2) % 4
    py = (me // 8) % 4
    pz = me // 32
    line = me // 8
    partner = me + 1 - 2 * core

    def at_x(i):
        return me + 2 * (i - px)

    def at_y(i):
        return me + 8 * (i - py)

    def at_z(i):
        return me + 32 * (i - pz)

    xcopies = [pltpu.make_async_copy(x.at[pl.ds(256 * i, 256)], xf.at[pl.ds(256 * i, 256)], xsem.at[i]) for i in range(8)]
    early = [(v, vv), (w0, w0v), (w1, w1v), (w2, w2v), (wu, wuv)]
    late = [
        (bu, buv), (b0, b0v), (b1, b1v), (b2, b2v),
        (wt.at[pl.ds(60 + 4 * line, 4)], wt6), (wt.at[pl.ds(28 + 2 * line, 2)], wt5),
        (wt.at[pl.ds(12 + 4 * pz, 4)], wt4), (wt.at[pl.ds(4 + 2 * pz, 2)], wt3), (wt.at[pl.ds(0, 4)], wt2),
        (bt.at[pl.ds(62 + 4 * line, 4)], bt6), (bt.at[pl.ds(30 + 2 * line, 2)], bt5),
        (bt.at[pl.ds(14 + line, 1)], bt4), (bt.at[pl.ds(6 + line // 2, 1)], bt3),
        (bt.at[pl.ds(2 + pz, 1)], bt2), (bt.at[pl.ds(pz // 2, 1)], bt1),
        (rt.at[pl.ds(60 + 4 * line, 4)], rt6), (rt.at[pl.ds(28 + 2 * line, 2)], rt5),
        (rt.at[pl.ds(12 + line, 1)], rt4), (rt.at[pl.ds(4 + line // 2, 1)], rt3), (rt.at[pl.ds(pz, 1)], rt2),
        (d, dv), (ru, ruv), (r2, r2v), (r1, r1v), (r0, r0v), (u, uv),
    ]
    ecopies = [pltpu.make_async_copy(a, b, lsem.at[i]) for i, (a, b) in enumerate(early)]
    lcopies = [pltpu.make_async_copy(a, b, wsem.at[i]) for i, (a, b) in enumerate(late)]
    ecopies[0].start()
    for c in xcopies:
        c.start()
    for c in ecopies[1:]:
        c.start()
    for c in lcopies:
        c.start()

    peers = [partner]
    for k in range(1, 4):
        peers += [at_x((px + k) % 4), at_y((py + k) % 4), at_z((pz + k) % 4)]
    barrier = pltpu.get_barrier_semaphore()
    for p in peers:
        pl.semaphore_signal(barrier, inc=1, device_id={'tree': p}, device_id_type=MESH)

    def send(src, dst, ssem, rsem, dev):
        c = pltpu.make_async_remote_copy(src_ref=src, dst_ref=dst, send_sem=ssem, recv_sem=rsem, device_id={'tree': dev}, device_id_type=MESH)
        c.start()
        return c

    ecopies[0].wait()
    for i in range(8):
        xcopies[i].wait()
        rows = pl.ds(256 * i, 256)
        xi = xf[rows, :].astype(BF16)
        xb[rows, :] = xi
        xh0[pl.ds(64 * i, 64), :] = nn(vv[i], xi).astype(BF16)
    for c in ecopies[1:]:
        c.wait()
    for n in range(4):
        xh1[pl.ds(128 * n, 128), :] = tn(w0v[2 * n:2 * n + 2].reshape(128, 128), xh0[pl.ds(128 * n, 128), :]).astype(BF16)
    for n in range(2):
        xh2[pl.ds(128 * n, 128), :] = tn(w1v[2 * n:2 * n + 2].reshape(256, 128), xh1[pl.ds(256 * n, 256), :]).astype(BF16)
    x7v = tn(w2v[...].reshape(256, 256), xh2[...]).astype(BF16)
    x7[0] = x7v[:, :256]
    x7[1] = x7v[:, 256:]

    part[...] = tn(x7[1 - core], wuv[0])
    pl.semaphore_wait(barrier, 10)
    c_part = send(part, partr, s0.at[0], q0.at[0], partner)
    c_skel = send(x7, x7s, s0.at[1], q0.at[1], partner)
    own = tn(x7[core], wuv[0])
    for c in lcopies:
        c.wait()
    c_part.wait_recv()
    x6h[...] = (own + partr[...]).astype(BF16).reshape(4, COLS, 256)

    c6 = [send(x6h.at[(px + k) % 4], buf6.at[px], s6.at[k - 1], q6.at[px], at_x((px + k) % 4)) for k in range(1, 4)]
    buf6[px] = x6h[px]

    def got(buf, sem, k, pos):
        src = (pos + k) % 4
        pltpu.make_async_remote_copy(src_ref=buf.at[src], dst_ref=buf.at[src], send_sem=sem.at[src], recv_sem=sem.at[src], device_id={'tree': partner}, device_id_type=MESH).wait_recv()

    for i in range(8):
        g0[pl.ds(64 * i, 64), :] = nn(b0v[i], xh0[pl.ds(64 * (i ^ 1), 64), :])
    for n in range(4):
        g1[pl.ds(128 * n, 128), :] = nn(b1v[n], xh1[pl.ds(128 * (n ^ 1), 128), :])
    for n in range(2):
        g2[pl.ds(128 * n, 128), :] = nn(b2v[n], xh2[pl.ds(128 * (1 - n), 128), :])

    def near(lo, hi):
        def step(i, carry):
            rows = pl.ds(pl.multiple_of(256 * i, 256), 256)
            out[rows, :] = nn(dv[i], xb[rows, :])
            return carry
        lax.fori_loop(lo, hi, step, 0)

    near(0, 3)
    for k in range(1, 4):
        got(buf6, q6, k, px)
    for j in range(2):
        x5[j] = (nn(buf6[2 * j], wt6[2 * j]) + nn(buf6[2 * j + 1], wt6[2 * j + 1])).astype(BF16)
    x4s[...] = (nn(x5[0], wt5[0]) + nn(x5[1], wt5[1])).astype(BF16)

    c4 = [send(x4s, buf4.at[py], s4.at[k - 1], q4.at[py], at_y((py + k) % 4)) for k in range(1, 4)]
    buf4[py] = x4s[...]
    for i in range(4):
        g6t[i] = nt(buf6[i ^ 1], bt6[i])
    for j in range(2):
        g5t[j] = nt(x5[1 - j], bt5[j])
    c_skel.wait_recv()
    for h in range(2):
        g7[:, pl.ds(256 * h, 256)] = nn(buv[0], x7s[h])
    near(3, 6)
    for k in range(1, 4):
        got(buf4, q4, k, py)
    for j in range(2):
        x3[j] = (nn(buf4[2 * j], wt4[2 * j]) + nn(buf4[2 * j + 1], wt4[2 * j + 1])).astype(BF16)
    x2s[...] = (nn(x3[0], wt3[0]) + nn(x3[1], wt3[1])).astype(BF16)

    c2 = [send(x2s, buf2.at[pz], s2.at[k - 1], q2.at[pz], at_z((pz + k) % 4)) for k in range(1, 4)]
    buf2[pz] = x2s[...]
    g4t = nt(buf4[py + 1 - 2 * (py % 2)], bt4[0])
    g3t = nt(x3[1 - py // 2], bt3[0])
    near(6, 8)
    for k in range(1, 4):
        got(buf2, q2, k, pz)
    for j in range(2):
        x1[j] = (nn(buf2[2 * j], wt2[2 * j]) + nn(buf2[2 * j + 1], wt2[2 * j + 1])).astype(BF16)
    g2t = nt(buf2[pz + 1 - 2 * (pz % 2)], bt2[0])

    y1 = nt(x1[1 - pz // 2], bt1[0]).astype(BF16)
    y2 = (g2t + nt(y1, rt2[0])).astype(BF16)
    y3 = (g3t + nt(y2, rt3[0])).astype(BF16)
    y4 = (g4t + nt(y3, rt4[0])).astype(BF16)
    y5 = [(g5t[j] + nt(y4, rt5[j])).astype(BF16) for j in range(2)]
    for i in range(4):
        y6h[i] = (g6t[i] + nt(y5[i // 2], rt6[i])).astype(BF16)

    cy = [send(y6h.at[(px + k) % 4], yfull.at[4 * core + px], sy.at[k - 1], qy.at[px], at_x((px + k) % 4)) for k in range(1, 4)]
    cc = [send(y6h.at[px], yfull.at[4 * core + px], sc.at[px], qc.at[px], partner)]
    yfull[4 * core + px] = y6h[px]
    for k in range(1, 4):
        src = (px + k) % 4
        slot = yfull.at[4 * core + src]
        pltpu.make_async_remote_copy(src_ref=slot, dst_ref=slot, send_sem=qy.at[src], recv_sem=qy.at[src], device_id={'tree': partner}, device_id_type=MESH).wait_recv()
        cc.append(send(slot, slot, sc.at[src], qc.at[src], partner))
    for i in range(4):
        slot = yfull.at[4 * (1 - core) + i]
        pltpu.make_async_remote_copy(src_ref=slot, dst_ref=slot, send_sem=qc.at[i], recv_sem=qc.at[i], device_id={'tree': partner}, device_id_type=MESH).wait_recv()

    y7 = (g7[...] + nt(ruv[0], yfull[...].reshape(512, 256))).astype(BF16)
    yh2 = [(g2[pl.ds(128 * n, 128), :] + nn(r2v[n], y7)).astype(BF16) for n in range(2)]
    yh1 = [(g1[pl.ds(128 * n, 128), :] + nn(r1v[n], yh2[n // 2])).astype(BF16) for n in range(4)]
    for i in range(8):
        yi = (g0[pl.ds(64 * i, 64), :] + nn(r0v[i], yh1[i // 2])).astype(BF16)
        out[pl.ds(256 * i, 256), :] += tn(uv[i], yi)

    for c in [c_part, c_skel] + c6 + c4 + c2 + cy + cc:
        c.wait_send()


def solution(mesh):
    rows_spec = P(('batch', 'tree'), None)
    tree_spec = P('tree', None, None)
    full_spec = P(None, None, None)

    def body(*args):
        args = list(args)
        for i in (2, 3):
            args[i] = jnp.swapaxes(args[i], 1, 2)
        args = [pltpu.with_memory_space_constraint(a, pltpu.HBM) for a in args]
        shapes = [a.shape for a in args]
        rows, cols = shapes[0]

        def b16(*shape):
            return pltpu.VMEM(shape, BF16)

        def f32(*shape):
            return pltpu.VMEM(shape, F32)

        dma = pltpu.SemaphoreType.DMA
        mat = (256, 256)
        scratch = [f32(rows, cols)] + [b16(rows, cols)] + [b16(*s) for s in shapes[1:16]]
        scratch += [b16(n, *mat) for n in (4, 2, 4, 2, 4, 4, 2, 1, 1, 1, 4, 2, 1, 1, 1, 1)]
        scratch += [b16(512, cols), b16(512, cols), b16(256, cols), b16(2, *mat), b16(2, *mat), f32(*mat), f32(*mat)]
        line = b16(4, COLS, 256)
        scratch += [line, line, b16(2, COLS, 256), b16(COLS, 256), line, b16(2, COLS, 256), b16(COLS, 256), line, b16(2, COLS, 256)]
        scratch += [f32(512, cols), f32(512, cols), f32(256, cols), f32(256, cols), f32(4, COLS, 256), f32(2, COLS, 256), line, b16(8, COLS, 256), b16(512, cols)]
        scratch += [dma((8,)), dma((5,)), dma((26,)), dma((2,)), dma((2,))]
        scratch += [dma((3,)), dma((4,))] * 4 + [dma((4,)), dma((4,))]
        return pl.pallas_call(
            kernel,
            out_shape=jax.ShapeDtypeStruct((rows, cols), F32),
            in_specs=[pl.BlockSpec(memory_space=pltpu.HBM)] * len(args),
            out_specs=pl.BlockSpec(memory_space=pltpu.VMEM),
            scratch_shapes=scratch,
            compiler_params=pltpu.CompilerParams(collective_id=0, has_side_effects=True, vmem_limit_bytes=40 * 1024 * 1024),
        )(*args)

    return jax.shard_map(body, mesh=mesh, in_specs=(rows_spec,) + (tree_spec,) * 15 + (full_spec,) * 3, out_specs=rows_spec, check_vma=False)
```
